32 devices in a mesh: kv: 2 (over x), bead: 16 (over z, y, core).
Axes of the slice: x: 2, y: 2, z: 4, core: 2. Of those that a mesh axis runs over, the one named last changes fastest.
Arguments:
- miller: int32 [3, 2048], P(None, 'kv'), may hold values from -40 to 40
- lattice_pos: int32 [3, 4096], P(None, ('kv', 'bead')), may hold values from 0 to 4095
- weights: float32 [32, 4096], P(None, ('kv', 'bead')), may hold values from -6 to 6
- observed: float32 [32, 2048], P(None, 'kv'), may hold values from 0.3 to 2
Outputs:
- grad_weights: float32 [32, 4096], P(None, ('kv', 'bead'))
- grad_positions: float32 [3, 4096], P(None, ('kv', 'bead'))
The draws below stay inside these ranges and needn't reach their ends.
All inputs are finite; a program needn't handle non-finite values.
Results may differ from the reference program's by a relative error of at most 0.0003.
Values sent between devices are 32-bit elements; how exact they have to be, the bound alone decides.
No kernel may reach another device: no remote copies, remote signals or barrier semaphores. Data moves between devices by JAX's collectives and lax.ppermute only.
A program may use at most 64 MiB of HBM per device.

```python
import math
import jax
import jax.numpy as jnp
from jax import lax

CHANNELS = 32
LATTICE = 4096
MILLER_MAX = 40
BOX_LEN = 64
BEADS = 4096
WAVES = 2048


def with_ends(result, key, low, high):
    extent = result.shape
    spot = [jax.random.randint(jax.random.fold_in(key, axis), (), 0, extent[axis]) for axis in range(len(extent))]
    result = result.at[tuple(spot)].set(low)
    longest = extent.index(max(extent))
    spot[longest] = (spot[longest] + 1) % extent[longest]
    return result.at[tuple(spot)].set(high)


def level_of(own_key, dims, split, low, high):
    level, own = 1.0, jax.random.fold_in(own_key, 6)
    for position, blocks in split:
        heights = jnp.exp(jax.random.uniform(jax.random.fold_in(own, position), (blocks,), jnp.float32, low / len(split), high / len(split)))
        level = level * jnp.repeat(heights, dims[position] // blocks).reshape([-1 if axis == position else 1 for axis in range(len(dims))])
    return level


def centred(rng, extent, spread, limit, cuts=(), dtype=jnp.bfloat16):
    array = jax.random.normal(rng, extent, jnp.float32) * spread
    if len(cuts) > 0:
        array = level_of(rng, extent, cuts, -0.22, 0.18) * array
    return jnp.clip(array, min=-limit, max=limit).astype(dtype)


def setup_inputs(seed: int = 0) -> dict:
    keys = jax.random.split(jax.random.key(seed), 5)
    miller = with_ends(jax.random.randint(keys[0], (3, WAVES), 0 - MILLER_MAX, MILLER_MAX + 1), jax.random.fold_in(keys[0], 1), 0 - MILLER_MAX, MILLER_MAX).astype(jnp.int32)
    lattice_pos = with_ends(jax.random.randint(keys[1], (3, BEADS), 0, LATTICE), jax.random.fold_in(keys[1], 1), 0, LATTICE - 1).astype(jnp.int32)
    weights = centred(keys[2], (CHANNELS, BEADS), 1.0, 6.0, ((1, 32),), jnp.float32)
    observed = jnp.clip(0.3 + 1.7 * jax.random.uniform(keys[3], (CHANNELS, WAVES), jnp.float32) ** level_of(keys[3], (CHANNELS, WAVES), ((1, 2),), -0.2, 0.2), 0.3, 2.0)
    return {"miller": miller, "lattice_pos": lattice_pos, "weights": weights, "observed": observed}


HIGH = lax.Precision.HIGHEST
TWO_PI = 2.0 * math.pi


def phases(mil_block, positions):
    integer = mil_block[0][:, None] * positions[0][None, :]
    integer = integer + mil_block[1][:, None] * positions[1][None, :]
    integer = integer + mil_block[2][:, None] * positions[2][None, :]
    return jnp.mod(integer, LATTICE).astype(jnp.float32) * (TWO_PI / LATTICE)


def reference(miller, lattice_pos, weights, observed):
    wave_count = miller.shape[1]
    block_size = math.gcd(wave_count, 512)
    count_blocks = wave_count // block_size
    mil_blocks = miller.reshape(3, count_blocks, block_size).transpose(1, 0, 2)

    def forward(mil_block):
        angles = phases(mil_block, lattice_pos)
        first = jnp.dot(weights, jnp.cos(angles).T, precision=HIGH, preferred_element_type=jnp.float32)
        second = jnp.dot(weights, jnp.sin(angles).T, precision=HIGH, preferred_element_type=jnp.float32)
        return first, second

    cos_blocks, sin_blocks = lax.map(forward, mil_blocks)
    amp_cos = cos_blocks.transpose(1, 0, 2).reshape(CHANNELS, wave_count)
    amp_sin = sin_blocks.transpose(1, 0, 2).reshape(CHANNELS, wave_count)
    bead_total = lattice_pos.shape[1]
    residual = (amp_cos * amp_cos + amp_sin * amp_sin) / bead_total - observed
    coef_cos = 2.0 * residual * amp_cos / bead_total
    coef_sin = 2.0 * residual * amp_sin / bead_total
    wave_vec = miller.astype(jnp.float32) * (TWO_PI / BOX_LEN)
    left_cos = jnp.concatenate([coef_cos] + [wave_vec[comp][None, :] * coef_sin for comp in range(3)], 0)
    left_sin = jnp.concatenate([coef_sin] + [-wave_vec[comp][None, :] * coef_cos for comp in range(3)], 0)
    left_cos = left_cos.reshape(4 * CHANNELS, count_blocks, block_size).transpose(1, 0, 2)
    left_sin = left_sin.reshape(4 * CHANNELS, count_blocks, block_size).transpose(1, 0, 2)

    def advance(running, pieces):
        mil_block, cos_left, sin_left = pieces
        angles = phases(mil_block, lattice_pos)
        running = running + jnp.dot(cos_left, jnp.cos(angles), precision=HIGH, preferred_element_type=jnp.float32)
        running = running + jnp.dot(sin_left, jnp.sin(angles), precision=HIGH, preferred_element_type=jnp.float32)
        return running, None

    start_total = jnp.zeros((4 * CHANNELS, bead_total), jnp.float32)
    summed, unused = lax.scan(advance, start_total, (mil_blocks, left_cos, left_sin))
    grad_weights = summed[:CHANNELS]
    grad_positions = jnp.stack([jnp.sum(weights * summed[CHANNELS * (comp + 1):CHANNELS * (comp + 2)], 0) for comp in range(3)])
    return grad_weights, grad_positions
```

```python
import math

import jax
import jax.numpy as jnp
from jax import lax
from jax.experimental import pallas as pl
from jax.experimental.pallas import tpu as pltpu
from jax.sharding import PartitionSpec as P

LATTICE = 4096
BOX_LEN = 64
LANES = 128
CHUNK = 256
ROWS = 16
AXES = ("kv", "bead")

C3 = -0.004594121399333958
G0, G1, G2 = -341.9144, 140.60645, -17.343199
W1 = 1.0 / C3**2
W2 = 0.5 / C3**2
SCALE = 8.0 * C3**4

F32 = jnp.float32
BF16 = jnp.bfloat16
VMEM = pl.BlockSpec(memory_space=pltpu.VMEM)


def split(value):
    high = value.astype(BF16)
    return high, (value - high.astype(F32)).astype(BF16)


def table(turns):
    r = turns - jnp.round(turns)
    z = r * r
    g = r * (((z + G2) * z + G1) * z + G0)
    a = g * g
    w = W1 - a
    return a * w, (g * (W2 - a)) * (w * lax.rsqrt(w))


def columns(chunk):
    return pl.ds(pl.multiple_of(chunk * CHUNK, CHUNK), CHUNK)


def amplitude_kernel(counts, waves, own, carried, final, *refs):
    refs = list(refs)
    blocks = [refs.pop(0) for _ in counts]
    m6_ref = refs.pop(0)
    acc_in, sum_in = (refs.pop(0), refs.pop(0)) if carried else (None, None)
    acc_ref = refs.pop(0)
    sum_ref = None if final else refs.pop(0)
    cos_out, sin_out = (refs.pop(0), refs.pop(0)) if own else (None, None)
    turned, parts, phase_a, phase_b, tab_a, tab_b = refs
    phase, tab = (phase_a, phase_b), (tab_a, tab_b)
    channels = acc_ref.shape[0] // 2
    number = sum(counts)
    chunks = waves // CHUNK
    steps = number * chunks

    total = sum_in[...] if carried else jnp.zeros((channels, LANES), F32)
    place = 0
    for block, count in zip(blocks, counts):
        for j in range(count):
            weight = block[j, 0:channels, :]
            high, low = split(weight)
            parts[place, 0:channels, :] = high
            parts[place, channels:, :] = low
            turned[place] = jnp.transpose(block[j, channels:, :])
            total = total + weight
            place += 1
    if not final:
        sum_ref[...] = total
    acc_ref[...] = acc_in[...] if carried else jnp.zeros_like(acc_ref)

    def phases(step, slot):
        m6 = m6_ref[:, columns(lax.rem(step, chunks))]
        phase[slot][...] = jnp.dot(turned[step // chunks], m6, preferred_element_type=F32)

    def trig(step, slot):
        for i in range(0, LANES, ROWS):
            cos, sin = table(phase[slot][i : i + ROWS, :])
            pieces = (*split(cos), *split(sin))
            for j, piece in enumerate(pieces):
                tab[slot][j, i : i + ROWS, :] = piece
            if own:
                there = columns(lax.rem(step, chunks))
                cos_out[i : i + ROWS, there] = pieces[0]
                cos_out[LANES + i : LANES + i + ROWS, there] = pieces[1]
                sin_out[i : i + ROWS, there] = pieces[2]
                sin_out[LANES + i : LANES + i + ROWS, there] = pieces[3]

    def gather(step, slot):
        there = columns(lax.rem(step, chunks))
        both = parts[step // chunks]
        high = both[0:channels]
        for q in range(2):
            on_high = jnp.dot(both, tab[slot][2 * q], preferred_element_type=F32)
            on_low = jnp.dot(high, tab[slot][2 * q + 1], preferred_element_type=F32)
            acc_ref[channels * q : channels * (q + 1), there] += (
                on_high[0:channels] + on_high[channels:] + on_low
            )

    phases(0, 0)
    phases(1, 1)
    trig(0, 0)

    def pair(i, unused):
        step = 1 + 2 * i
        phases(step + 1, 0)
        trig(step, 1)
        gather(step - 1, 0)
        phases(step + 2, 1)
        trig(step + 1, 0)
        gather(step, 1)
        return unused

    lax.fori_loop(0, (steps - 2) // 2, pair, 0)
    trig(steps - 1, 1)
    gather(steps - 2, 0)
    gather(steps - 1, 1)
    if final:
        whole = jnp.sum(total, axis=1, keepdims=True)
        acc_ref[0:channels, :] = whole - SCALE * acc_ref[0:channels, :]
        acc_ref[channels:, :] = -SCALE * acc_ref[channels:, :]


def amplitudes(blocks, m6, channels, carry=None, own=False, final=False):
    waves = m6.shape[1]
    counts = tuple(b.shape[0] for b in blocks)
    number = sum(counts)
    outs = [jax.ShapeDtypeStruct((2 * channels, waves), F32)]
    if not final:
        outs.append(jax.ShapeDtypeStruct((channels, LANES), F32))
    if own:
        outs += [jax.ShapeDtypeStruct((2 * LANES, waves), BF16)] * 2
    args = (*blocks, m6, *(carry or ()))
    work = number * LANES * waves

    def body(*refs):
        amplitude_kernel(counts, waves, own, carry is not None, final, *refs)

    return pl.pallas_call(
        body,
        out_shape=outs,
        in_specs=[VMEM] * len(args),
        out_specs=[VMEM] * len(outs),
        scratch_shapes=[
            pltpu.VMEM((number, LANES, 8), F32),
            pltpu.VMEM((number, 2 * channels, LANES), BF16),
            pltpu.VMEM((LANES, CHUNK), F32),
            pltpu.VMEM((LANES, CHUNK), F32),
            pltpu.VMEM((4, LANES, CHUNK), BF16),
            pltpu.VMEM((4, LANES, CHUNK), BF16),
        ],
        cost_estimate=pl.CostEstimate(flops=work * 200, bytes_accessed=8 * waves * channels, transcendentals=work),
        name="own_amplitudes" if own else "amplitudes",
    )(*args)


def gradient_kernel(kv, local, bead_total, *refs):
    refs = list(refs)
    mine, other = refs.pop(0), refs.pop(0)
    measured = [refs.pop(0) for _ in range(kv)]
    m6_ref, cos_tab, sin_tab, weights = (refs.pop(0) for _ in range(4))
    grad_w, grad_p, cos_left, sin_left = refs
    channels = weights.shape[0]
    waves = kv * local
    rows = 4 * channels
    constant = jnp.zeros((rows, CHUNK), F32)
    for start in range(0, waves, CHUNK):
        part, inside = start // local, start % local
        span = slice(start, start + CHUNK)
        cos = mine[0:channels, span] + other[0:channels, span]
        sin = mine[channels:, span] + other[channels:, span]
        residual = (cos * cos + sin * sin) * (1.0 / bead_total) - measured[part][:, inside : inside + CHUNK]
        factor = residual * (2.0 / bead_total)
        cos, sin = factor * cos, factor * sin
        m = [m6_ref[d : d + 1, span] for d in range(3)]
        on_cos = jnp.concatenate([cos] + [m[d] * sin for d in range(3)], 0)
        on_sin = jnp.concatenate([sin] + [-m[d] * cos for d in range(3)], 0)
        constant = constant + on_cos
        cos_left[0:rows, span], cos_left[rows:, span] = split(on_cos)
        sin_left[0:rows, span], sin_left[rows:, span] = split(on_sin)
    contract = (((1,), (1,)), ((), ()))
    both = lax.dot_general(cos_left[...], cos_tab[...], contract, preferred_element_type=F32)
    both = both + lax.dot_general(sin_left[...], sin_tab[...], contract, preferred_element_type=F32)
    both = both[0:rows, 0:LANES] + both[0:rows, LANES:] + both[rows:, 0:LANES]
    result = jnp.sum(constant, axis=1, keepdims=True) - SCALE * both
    grad_w[...] = result[0:channels]
    for d in range(3):
        piece = weights[...] * result[channels * (d + 1) : channels * (d + 2)]
        grad_p[d : d + 1, :] = jnp.sum(piece, axis=0, keepdims=True) * (2.0 * math.pi / BOX_LEN)


def gradients(mine, other, measured, m6, cos_tab, sin_tab, weights, bead_total):
    channels, waves = weights.shape[0], m6.shape[1]
    args = (mine, other, *measured, m6, cos_tab, sin_tab, weights)

    def body(*refs):
        gradient_kernel(len(measured), waves // len(measured), bead_total, *refs)

    return pl.pallas_call(
        body,
        out_shape=[jax.ShapeDtypeStruct((channels, LANES), F32), jax.ShapeDtypeStruct((3, LANES), F32)],
        in_specs=[VMEM] * len(args),
        out_specs=[VMEM] * 2,
        scratch_shapes=[pltpu.VMEM((8 * channels, waves), BF16)] * 2,
        cost_estimate=pl.CostEstimate(flops=16 * LANES * channels * waves, bytes_accessed=8 * waves * channels, transcendentals=0),
        name="gradients",
    )(*args)


def per_device(miller, lattice_pos, weights, observed):
    kv, beads = lax.axis_size("kv"), lax.axis_size("bead")
    devices = kv * beads
    channels = weights.shape[0]
    bead_total = weights.shape[1] * devices

    def exchange(value, mask):
        return lax.ppermute(value, AXES, [(i, i ^ mask) for i in range(devices)])

    def six(mil):
        rows = mil.astype(F32)
        return jnp.concatenate([rows, rows, jnp.zeros((2, mil.shape[1]), F32)], 0)

    fine = 1.0 / LATTICE
    upper = lattice_pos // 64
    lower = lattice_pos - 64 * upper
    block = jnp.concatenate(
        [
            weights,
            upper.astype(F32) * (64 * fine),
            lower.astype(F32) * fine,
            jnp.zeros((2, weights.shape[1]), F32),
        ],
        0,
    )[None]

    masks = [beads << j for j in range((kv - 1).bit_length())]
    masks += [1 << j for j in range(1, (beads - 1).bit_length())]
    stages = [masks[i : i + 2] for i in range(0, len(masks), 2)]

    millers = [miller] + [exchange(miller, beads * j) for j in range(1, kv)]
    m6 = jnp.concatenate([six(m) for m in millers], 1)
    *carry, cos_tab, sin_tab = amplitudes([block], m6, channels, own=True)
    held = block
    for number, stage in enumerate(stages):
        steps = stage if len(stage) == 1 else [stage[1], stage[0], stage[0] ^ stage[1]]
        arrived = [exchange(held, mask) for mask in steps]
        if number == 0:
            measured = [observed] + [exchange(observed, beads * j) for j in range(1, kv)]
        last = number == len(stages) - 1
        carry = amplitudes(arrived, m6, channels, carry=carry, final=last)
        if not last:
            held = jnp.concatenate([held, *arrived], 0)
    mine = carry[0]
    other = exchange(mine, 1)
    return tuple(gradients(mine, other, measured, m6, cos_tab, sin_tab, weights, bead_total))


def solution(mesh):
    in_specs = (P(None, "kv"), P(None, ("kv", "bead")), P(None, ("kv", "bead")), P(None, "kv"))
    out_specs = (P(None, ("kv", "bead")), P(None, ("kv", "bead")))
    return jax.shard_map(
        per_device, mesh=mesh, in_specs=in_specs, out_specs=out_specs, check_vma=False
    )
```

```python
import math

import jax
import jax.numpy as jnp
from jax import lax
from jax.experimental import pallas as pl
from jax.experimental.pallas import tpu as pltpu
from jax.sharding import PartitionSpec as P

LATTICE = 4096
BOX_LEN = 64
LANES = 128
CHUNK = 256
ROWS = 16
AXES = ("kv", "bead")
GRANT = 16 * 2**20

C3 = -0.004594121399333958
G0, G1, G2 = -341.9144, 140.60645, -17.343199
W1 = 1.0 / C3**2
W2 = 0.5 / C3**2
SCALE = 8.0 * C3**4

F32 = jnp.float32
BF16 = jnp.bfloat16
VMEM = pl.BlockSpec(memory_space=pltpu.VMEM)


def split(value):
    high = value.astype(BF16)
    return high, (value - high.astype(F32)).astype(BF16)


def table(turns):
    r = turns - jnp.round(turns)
    z = r * r
    g = r * (((z + G2) * z + G1) * z + G0)
    a = g * g
    w = W1 - a
    return a * w, (g * (W2 - a)) * (w * lax.rsqrt(w))


def columns(chunk):
    return pl.ds(pl.multiple_of(chunk * CHUNK, CHUNK), CHUNK)


def pack_kernel(weights, lattice_pos, block):
    channels = weights.shape[0]
    block[0, 0:channels, :] = weights[...]
    place = lattice_pos[...]
    block[0, channels : channels + 3, :] = (place >> 6).astype(F32) * (64.0 / LATTICE)
    block[0, channels + 3 : channels + 6, :] = (place & 63).astype(F32) * (1.0 / LATTICE)
    block[0, channels + 6 : channels + 8, :] = jnp.zeros((2, LANES), F32)


def pack(weights, lattice_pos):
    return pl.pallas_call(
        pack_kernel,
        out_shape=jax.ShapeDtypeStruct((1, weights.shape[0] + 8, LANES), F32),
        in_specs=[VMEM] * 2,
        out_specs=VMEM,
        compiler_params=pltpu.CompilerParams(vmem_limit_bytes=GRANT),
        name="pack",
    )(weights, lattice_pos)


def amplitude_kernel(counts, saved, carried, final, *refs):
    refs = list(refs)
    blocks = [refs.pop(0) for _ in counts]
    miller = refs.pop(0)
    acc_in, sum_in = (refs.pop(0), refs.pop(0)) if carried else (None, None)
    acc_ref = refs.pop(0)
    sum_ref = None if final else refs.pop(0)
    cos_out, sin_out = (refs.pop(0), refs.pop(0)) if saved else (None, None)
    m6_ref, turned, parts, phase_a, phase_b, tab_a, tab_b = refs
    phase, tab = (phase_a, phase_b), (tab_a, tab_b)
    channels = acc_ref.shape[0] // 2
    waves = acc_ref.shape[1]
    number = sum(counts)
    chunks = waves // CHUNK

    m = miller[...].astype(F32)
    m6_ref[0:3, :] = m
    m6_ref[3:6, :] = m
    m6_ref[6:8, :] = jnp.zeros((2, waves), F32)
    total = sum_in[...] if carried else jnp.zeros((channels, LANES), F32)
    place = 0
    for block, count in zip(blocks, counts):
        for j in range(count):
            weight = block[j, 0:channels, :]
            high, low = split(weight)
            parts[place, 0:channels, :] = high
            parts[place, channels:, :] = low
            turned[place] = jnp.transpose(block[j, channels:, :])
            total = total + weight
            place += 1
    if not final:
        sum_ref[...] = total
    acc_ref[...] = acc_in[...] if carried else jnp.zeros_like(acc_ref)

    def phases(step, slot):
        m6 = m6_ref[:, columns(lax.rem(step, chunks))]
        phase[slot][...] = jnp.dot(turned[step // chunks], m6, preferred_element_type=F32)

    def trig(step, slot, save):
        for i in range(0, LANES, ROWS):
            cos, sin = table(phase[slot][i : i + ROWS, :])
            pieces = (*split(cos), *split(sin))
            for j, piece in enumerate(pieces):
                tab[slot][j, i : i + ROWS, :] = piece
            if save:
                n, there = step // chunks, columns(lax.rem(step, chunks))
                cos_out[n, i : i + ROWS, there] = pieces[0]
                cos_out[n, LANES + i : LANES + i + ROWS, there] = pieces[1]
                sin_out[n, i : i + ROWS, there] = pieces[2]
                sin_out[n, LANES + i : LANES + i + ROWS, there] = pieces[3]

    def gather(step, slot):
        there = columns(lax.rem(step, chunks))
        both = parts[step // chunks]
        high = both[0:channels]
        for q in range(2):
            on_high = jnp.dot(both, tab[slot][2 * q], preferred_element_type=F32)
            on_low = jnp.dot(high, tab[slot][2 * q + 1], preferred_element_type=F32)
            acc_ref[channels * q : channels * (q + 1), there] += (
                on_high[0:channels] + on_high[channels:] + on_low
            )

    def run(first, last, save):
        phases(first, 0)
        phases(first + 1, 1)
        trig(first, 0, save)

        def pair(i, unused):
            step = first + 1 + 2 * i
            phases(step + 1, 0)
            trig(step, 1, save)
            gather(step - 1, 0)
            phases(step + 2, 1)
            trig(step + 1, 0, save)
            gather(step, 1)
            return unused

        lax.fori_loop(0, (last - first - 2) // 2, pair, 0)
        trig(last - 1, 1, save)
        gather(last - 2, 0)
        gather(last - 1, 1)

    if saved:
        run(0, saved * chunks, True)
    if saved < number:
        run(saved * chunks, number * chunks, False)
    if final:
        whole = jnp.sum(total, axis=1, keepdims=True)
        acc_ref[0:channels, :] = whole - SCALE * acc_ref[0:channels, :]
        acc_ref[channels:, :] = -SCALE * acc_ref[channels:, :]


def amplitudes(blocks, miller, channels, carry=None, saved=0, final=False):
    waves = miller.shape[1]
    counts = tuple(b.shape[0] for b in blocks)
    number = sum(counts)
    outs = [jax.ShapeDtypeStruct((2 * channels, waves), F32)]
    if not final:
        outs.append(jax.ShapeDtypeStruct((channels, LANES), F32))
    if saved:
        outs += [jax.ShapeDtypeStruct((saved, 2 * LANES, waves), BF16)] * 2
    args = (*blocks, miller, *(carry or ()))
    work = number * LANES * waves

    def body(*refs):
        amplitude_kernel(counts, saved, carry is not None, final, *refs)

    return pl.pallas_call(
        body,
        out_shape=outs,
        in_specs=[VMEM] * len(args),
        out_specs=[VMEM] * len(outs),
        scratch_shapes=[
            pltpu.VMEM((8, waves), F32),
            pltpu.VMEM((number, LANES, 8), F32),
            pltpu.VMEM((number, 2 * channels, LANES), BF16),
            pltpu.VMEM((LANES, CHUNK), F32),
            pltpu.VMEM((LANES, CHUNK), F32),
            pltpu.VMEM((4, LANES, CHUNK), BF16),
            pltpu.VMEM((4, LANES, CHUNK), BF16),
        ],
        compiler_params=pltpu.CompilerParams(vmem_limit_bytes=GRANT),
        cost_estimate=pl.CostEstimate(flops=work * 200, bytes_accessed=8 * waves * channels, transcendentals=work),
        name="amplitudes",
    )(*args)


def gradient_kernel(bead_total, *refs):
    refs = list(refs)
    mine, other, measured, miller, cos_tab, sin_tab = (refs.pop(0) for _ in range(6))
    owners = cos_tab.shape[0]
    weights = [refs.pop(0) for _ in range(owners)]
    results = [refs.pop(0) for _ in range(owners)]
    cos_left, sin_left = refs
    channels, waves = measured.shape
    rows = 4 * channels
    constant = jnp.zeros((rows, CHUNK), F32)
    for start in range(0, waves, CHUNK):
        span = slice(start, start + CHUNK)
        cos = mine[0:channels, span] + other[0:channels, span]
        sin = mine[channels:, span] + other[channels:, span]
        residual = (cos * cos + sin * sin) * (1.0 / bead_total) - measured[:, span]
        factor = residual * (2.0 / bead_total)
        cos, sin = factor * cos, factor * sin
        m = miller[:, span].astype(F32)
        m = [m[d : d + 1] for d in range(3)]
        on_cos = jnp.concatenate([cos] + [m[d] * sin for d in range(3)], 0)
        on_sin = jnp.concatenate([sin] + [-m[d] * cos for d in range(3)], 0)
        constant = constant + on_cos
        cos_left[0:rows, span], cos_left[rows:, span] = split(on_cos)
        sin_left[0:rows, span], sin_left[rows:, span] = split(on_sin)
    contract = (((1,), (1,)), ((), ()))
    constant = jnp.sum(constant, axis=1, keepdims=True)
    for n in range(owners):
        both = lax.dot_general(cos_left[...], cos_tab[n], contract, preferred_element_type=F32)
        both = both + lax.dot_general(sin_left[...], sin_tab[n], contract, preferred_element_type=F32)
        both = both[0:rows, 0:LANES] + both[0:rows, LANES:] + both[rows:, 0:LANES]
        result = constant - SCALE * both
        results[n][0:channels, :] = result[0:channels]
        for d in range(3):
            piece = weights[n][0, 0:channels, :] * result[channels * (d + 1) : channels * (d + 2)]
            total = jnp.sum(piece, axis=0, keepdims=True) * (2.0 * math.pi / BOX_LEN)
            results[n][channels + d : channels + d + 1, :] = total
        results[n][channels + 3 :, :] = jnp.zeros((5, LANES), F32)


def gradients(mine, other, measured, miller, cos_tab, sin_tab, blocks, bead_total):
    channels, waves = measured.shape
    args = (mine, other, measured, miller, cos_tab, sin_tab, *blocks)

    def body(*refs):
        gradient_kernel(bead_total, *refs)

    return pl.pallas_call(
        body,
        out_shape=[jax.ShapeDtypeStruct((channels + 8, LANES), F32)] * len(blocks),
        in_specs=[VMEM] * len(args),
        out_specs=[VMEM] * len(blocks),
        scratch_shapes=[pltpu.VMEM((8 * channels, waves), BF16)] * 2,
        compiler_params=pltpu.CompilerParams(vmem_limit_bytes=GRANT),
        cost_estimate=pl.CostEstimate(
            flops=16 * LANES * channels * waves * len(blocks), bytes_accessed=8 * waves * channels, transcendentals=0
        ),
        name="gradients",
    )(*args)


def per_device(miller, lattice_pos, weights, observed):
    kv, beads = lax.axis_size("kv"), lax.axis_size("bead")
    devices = kv * beads
    channels = weights.shape[0]
    bead_total = weights.shape[1] * devices

    def exchange(value, mask):
        return lax.ppermute(value, AXES, [(i, i ^ mask) for i in range(devices)])

    masks = [beads << j for j in range((kv - 1).bit_length())]
    masks += [1 << j for j in range(1, (beads - 1).bit_length())]
    held = {0: pack(weights, lattice_pos)}
    partners = [beads * j for j in range(kv)]
    blocks, waiting, carry, tables = [], dict(held), None, None
    stack, members = held[0], [0]
    for place in range(0, len(masks), 2):
        stage = masks[place : place + 2]
        steps = stage if len(stage) == 1 else [stage[1], stage[0], stage[0] ^ stage[1]]
        arrived = {mask: exchange(stack, mask) for mask in steps}
        last = place + 2 >= len(masks)
        for mask, value in arrived.items():
            for j, member in enumerate(members):
                if member ^ mask in partners:
                    waiting[member ^ mask] = value[j : j + 1]
        ready = all(p in waiting for p in partners)
        rest = list(arrived.values())
        if tables is None and ready:
            whole = [v for m, v in arrived.items() if not any(k ^ m in partners for k in members)]
            loose = [
                v[j : j + 1]
                for m, v in arrived.items()
                if any(k ^ m in partners for k in members)
                for j, k in enumerate(members)
                if k ^ m not in partners
            ]
            own = [waiting[p] for p in partners]
            if carry is None:
                before = [v[None] for j, v in enumerate(stack) if members[j] not in partners]
                loose = before + loose
            out = amplitudes(own + whole + loose, miller, channels, saved=len(own))
            carry, tables = out[:2], out[2:]
        elif tables is not None:
            carry = amplitudes(rest, miller, channels, carry=carry, final=last)
        members = members + [k ^ m for m in steps for k in members]
        if not last:
            stack = jnp.concatenate([stack, *rest], 0)
    mine = carry[0]
    other = exchange(mine, 1)
    mine, *theirs = gradients(
        mine, other, observed, miller, *tables, [waiting[p] for p in partners], bead_total
    )
    for j, value in enumerate(theirs):
        mine = mine + exchange(value, beads * (j + 1))
    return (mine[0:channels], mine[channels : channels + 3])


def solution(mesh):
    in_specs = (P(None, "kv"), P(None, ("kv", "bead")), P(None, ("kv", "bead")), P(None, "kv"))
    out_specs = (P(None, ("kv", "bead")), P(None, ("kv", "bead")))
    return jax.shard_map(
        per_device, mesh=mesh, in_specs=in_specs, out_specs=out_specs, check_vma=False
    )
```

```python
import math

import jax
import jax.numpy as jnp
from jax import lax
from jax.experimental import pallas as pl
from jax.experimental.pallas import tpu as pltpu
from jax.sharding import PartitionSpec as P

LATTICE = 4096
BOX_LEN = 64
LANES = 128
CHUNK = 256
ROWS = 16
TILE = 1
AHEAD = 2
DEPTH = 1
FLAGS = {}
HALVED = True
MERGE = 1
AXES = ("kv", "bead")
GRANT = 16 * 2**20

C3 = -0.004594121399333958
G0, G1, G2 = -341.9144, 140.60645, -17.343199
W1 = 1.0 / C3**2
W2 = 0.5 / C3**2
SCALE = 8.0 * C3**4

F32 = jnp.float32
BF16 = jnp.bfloat16
VMEM = pl.BlockSpec(memory_space=pltpu.VMEM)


def split(value):
    high = value.astype(BF16)
    return high, (value - high.astype(F32)).astype(BF16)


def table(turns):
    r = turns - jnp.round(turns)
    z = r * r
    g = r * (((z + G2) * z + G1) * z + G0)
    a = g * g
    w = W1 - a
    return a * w, (g * (W2 - a)) * (w * lax.rsqrt(w))


def columns(chunk):
    return pl.ds(pl.multiple_of(chunk * CHUNK, CHUNK), CHUNK)


def half_of(ref):
    if not HALVED:
        return ref[...]
    width = ref.shape[1] // 2
    second = lax.rem(lax.axis_index("bead") // 2, 2)
    return ref[:, pl.ds(pl.multiple_of(second * width, width), width)]


def six_rows(rows):
    upper = jnp.floor(rows * (1.0 / 64.0))
    lower = rows - 64.0 * upper
    return upper * (64.0 / LATTICE) + pltpu.roll(lower * (1.0 / LATTICE), 3, 0)


def amplitude_kernel(counts, carried, final, *refs):
    refs = list(refs)
    held = [refs.pop(0) for _ in counts]
    blocks = [(ref, j) for ref, count in zip(held, counts) for j in range(count)]
    miller = refs.pop(0)
    acc_in, sum_in = (refs.pop(0), refs.pop(0)) if carried else (None, None)
    acc_ref = refs.pop(0)
    sum_ref = None if final else refs.pop(0)
    *tables, m6_ref, turned, parts, phase = refs
    channels, waves = acc_ref.shape[0] // 2, acc_ref.shape[1]
    number = len(blocks)

    m = half_of(miller).astype(F32)
    m6_ref[0:3, :] = m
    m6_ref[3:6, :] = m
    m6_ref[6:8, :] = jnp.zeros((2, waves), F32)
    total = sum_in[...] if carried else jnp.zeros((channels, LANES), F32)
    for place, (ref, j) in enumerate(blocks):
        rows = slice(LANES * place, LANES * (place + 1))
        weight = ref[j, 0:channels, :]
        parts[0:channels, rows], parts[channels:, rows] = split(weight)
        turned[rows, :] = jnp.transpose(six_rows(ref[j, channels:, :]))
        total = total + weight
    if not final:
        sum_ref[...] = total
    whole = jnp.sum(total, axis=1, keepdims=True) if final else None

    def phases(step):
        rows, there = step
        phase[rows, there] = jnp.dot(turned[rows, :], m6_ref[:, there], preferred_element_type=F32)

    def trig(step):
        rows, there = step
        for i in range(rows.start, rows.stop, ROWS):
            cos, sin = table(phase[i : i + ROWS, there])
            for ref, piece in zip(tables, (*split(cos), *split(sin))):
                ref[i : i + ROWS, there] = piece

    def gather(rows, there, sums):
        both = parts[:, rows]
        for q in range(2):
            on_high = jnp.dot(both, tables[2 * q][rows, there], preferred_element_type=F32)
            on_low = jnp.dot(both[0:channels], tables[2 * q + 1][rows, there], preferred_element_type=F32)
            sums[2 * q] = on_high if sums[2 * q] is None else sums[2 * q] + on_high
            sums[2 * q + 1] = on_low if sums[2 * q + 1] is None else sums[2 * q + 1] + on_low

    def finish(there, sums):
        for q in range(2):
            out = slice(channels * q, channels * (q + 1))
            value = sums[2 * q][0:channels] + sums[2 * q][channels:] + sums[2 * q + 1]
            if carried:
                value = value + acc_in[out, there]
            if final:
                value = -SCALE * value if q else whole - SCALE * value
            acc_ref[out, there] = value

    spans = [slice(c, c + CHUNK) for c in range(0, waves, CHUNK)]
    tile = TILE * LANES
    steps = [(slice(r, r + tile), there) for there in spans for r in range(0, number * LANES, tile)]
    for step in steps[:AHEAD]:
        phases(step)
    sums = [None] * 4
    done = 0
    for n, (rows, there) in enumerate(steps):
        if n + AHEAD < len(steps):
            phases(steps[n + AHEAD])
        trig((rows, there))
        if (rows.stop - done) >= DEPTH * LANES or rows.stop == number * LANES:
            gather(slice(done, rows.stop), there, sums)
            done = rows.stop
        if rows.stop == number * LANES:
            finish(there, sums)
            sums, done = [None] * 4, 0


def amplitudes(blocks, miller, channels, carry=None, final=False):
    waves = miller.shape[1] // (2 if HALVED else 1)
    counts = tuple(b.shape[0] for b in blocks)
    number = sum(counts)
    outs = [jax.ShapeDtypeStruct((2 * channels, waves), F32)]
    if not final:
        outs.append(jax.ShapeDtypeStruct((channels, LANES), F32))
    outs += [jax.ShapeDtypeStruct((number * LANES, waves), BF16)] * 4
    args = (*blocks, miller, *(carry or ()))
    work = number * LANES * waves

    def body(*refs):
        amplitude_kernel(counts, carry is not None, final, *refs)

    out = pl.pallas_call(
        body,
        out_shape=outs,
        in_specs=[VMEM] * len(args),
        out_specs=[VMEM] * len(outs),
        scratch_shapes=[
            pltpu.VMEM((8, waves), F32),
            pltpu.VMEM((number * LANES, 8), F32),
            pltpu.VMEM((2 * channels, number * LANES), BF16),
            pltpu.VMEM((number * LANES, waves), F32),
        ],
        compiler_params=pltpu.CompilerParams(vmem_limit_bytes=GRANT, flags=FLAGS),
        cost_estimate=pl.CostEstimate(flops=work * 200, bytes_accessed=8 * waves * channels, transcendentals=work),
        name="amplitudes",
    )(*args)
    return out[:-4], out[-4:]


def gradient_kernel(bead_total, places, *refs):
    owners = len(places)
    refs = list(refs)
    mine, other, measured, miller = (refs.pop(0) for _ in range(4))
    weights = [refs.pop(0) for _ in range(owners)]
    tables = [[refs.pop(0) for _ in range(4)] for _ in range(owners)]
    results = [refs.pop(0) for _ in range(owners)]
    cos_left, sin_left = refs
    channels, waves = mine.shape[0] // 2, mine.shape[1]
    goal, indices = half_of(measured), half_of(miller).astype(F32)
    rows = 4 * channels
    constant = jnp.zeros((rows, CHUNK), F32)
    for start in range(0, waves, CHUNK):
        span = slice(start, start + CHUNK)
        cos = mine[0:channels, span] + other[0:channels, span]
        sin = mine[channels:, span] + other[channels:, span]
        residual = (cos * cos + sin * sin) * (1.0 / bead_total) - goal[:, span]
        factor = residual * (2.0 / bead_total)
        cos, sin = factor * cos, factor * sin
        m = [indices[d : d + 1, span] for d in range(3)]
        on_cos = jnp.concatenate([cos] + [m[d] * sin for d in range(3)], 0)
        on_sin = jnp.concatenate([sin] + [-m[d] * cos for d in range(3)], 0)
        constant = constant + on_cos
        cos_left[0:rows, span], cos_left[rows:, span] = split(on_cos)
        sin_left[0:rows, span], sin_left[rows:, span] = split(on_sin)
    contract = (((1,), (1,)), ((), ()))
    constant = jnp.sum(constant, axis=1, keepdims=True)
    for n in range(owners):
        cos_high, cos_low, sin_high, sin_low = (t[places[n][1] * LANES : (places[n][1] + 1) * LANES, :] for t in tables[n])
        both = lax.dot_general(cos_left[...], cos_high, contract, preferred_element_type=F32)
        both = both + lax.dot_general(sin_left[...], sin_high, contract, preferred_element_type=F32)
        low = lax.dot_general(cos_left[0:rows], cos_low, contract, preferred_element_type=F32)
        low = low + lax.dot_general(sin_left[0:rows], sin_low, contract, preferred_element_type=F32)
        both = both[0:rows] + both[rows:] + low
        result = constant - SCALE * both
        results[n][0:channels, :] = result[0:channels]
        for d in range(3):
            piece = weights[n][places[n][0], 0:channels, :] * result[channels * (d + 1) : channels * (d + 2)]
            total = jnp.sum(piece, axis=0, keepdims=True) * (2.0 * math.pi / BOX_LEN)
            results[n][channels + d : channels + d + 1, :] = total
        results[n][channels + 3 :, :] = jnp.zeros((5, LANES), F32)


def gradients(mine, other, measured, miller, blocks, tables, places, bead_total):
    channels, waves = mine.shape[0] // 2, mine.shape[1]
    args = (mine, other, measured, miller, *blocks, *tables)

    def body(*refs):
        gradient_kernel(bead_total, places, *refs)

    return pl.pallas_call(
        body,
        out_shape=[jax.ShapeDtypeStruct((channels + 8, LANES), F32)] * len(blocks),
        in_specs=[VMEM] * len(args),
        out_specs=[VMEM] * len(blocks),
        scratch_shapes=[pltpu.VMEM((8 * channels, waves), BF16)] * 2,
        compiler_params=pltpu.CompilerParams(vmem_limit_bytes=GRANT),
        cost_estimate=pl.CostEstimate(
            flops=16 * LANES * channels * waves * len(blocks), bytes_accessed=8 * waves * channels, transcendentals=0
        ),
        name="gradients",
    )(*args)


def total_kernel(*refs):
    *terms, grad_weights, grad_positions = refs
    channels = grad_weights.shape[0]
    total = terms[0][...]
    for term in terms[1:]:
        total = total + term[...]
    grad_weights[...] = total[0:channels]
    grad_positions[...] = total[channels : channels + 3]


def total_of(terms, channels):
    return pl.pallas_call(
        total_kernel,
        out_shape=[jax.ShapeDtypeStruct((channels, LANES), F32), jax.ShapeDtypeStruct((3, LANES), F32)],
        in_specs=[VMEM] * len(terms),
        out_specs=[VMEM] * 2,
        compiler_params=pltpu.CompilerParams(vmem_limit_bytes=GRANT),
        name="total",
    )(*terms)


def steps_of(masks):
    stages = [masks[i : i + 2] for i in range(0, len(masks), 2)]
    return [[m | 1 for m in (s if len(s) == 1 else (s[0], s[1], s[0] | s[1]))] for s in stages]


def per_device(miller, lattice_pos, weights, observed):
    kv, beads = lax.axis_size("kv"), lax.axis_size("bead")
    devices = kv * beads
    channels = weights.shape[0]
    bead_total = weights.shape[1] * devices

    def exchange(value, mask):
        return lax.ppermute(value, AXES, [(i, i ^ mask) for i in range(devices)])

    cut = [beads << j for j in range((kv - 1).bit_length())] + ([2] if HALVED else [])
    rest = [1 << j for j in reversed(range(1, (beads - 1).bit_length())) if 1 << j not in cut]
    block = jnp.pad(weights, ((0, 8), (0, 0))) + jnp.pad(
        lattice_pos, ((channels, 5), (0, 0))
    ).astype(F32)
    stack, members, stages = block[None], [0], steps_of(rest + cut)
    for step in stages[:-1]:
        stack = jnp.concatenate([stack, *(exchange(stack, mask) for mask in step)], 0)
        members += [k ^ mask for mask in step for k in members]
    arrived = [(0, stack)] + [(mask, exchange(stack, mask)) for mask in stages[-1]]
    few = min(len(members), 4)
    groups = [[(mask, value, j)] for mask, value in arrived for j in range(0, len(members), few)]
    if MERGE > 1 and len(groups) > MERGE:
        groups[-MERGE:] = [sum(groups[-MERGE:], [])]
    carry, tables, owned = None, [], []
    for group in groups:
        parts = [value[j : j + few] for _, value, j in group]
        carry, saved = amplitudes(parts, miller, channels, carry=carry, final=group is groups[-1])
        for n, (mask, _, j) in enumerate(group):
            for k in range(few):
                owner = members[j + k] ^ mask
                if all(owner & bit == 0 for bit in rest):
                    owned.append((owner, parts[n], (k, n * few + k)))
                    tables += saved
    mine = carry[0]
    results = gradients(
        mine,
        exchange(mine, 1),
        observed,
        miller,
        [part for _, part, _ in owned],
        tables,
        [place for _, _, place in owned],
        bead_total,
    )
    terms = [exchange(r, owner) if owner else r for (owner, _, _), r in zip(owned, results)]
    return tuple(total_of(terms, channels))


def solution(mesh):
    in_specs = (P(None, "kv"), P(None, ("kv", "bead")), P(None, ("kv", "bead")), P(None, "kv"))
    out_specs = (P(None, ("kv", "bead")), P(None, ("kv", "bead")))
    return jax.shard_map(
        per_device, mesh=mesh, in_specs=in_specs, out_specs=out_specs, check_vma=False
    )
```
